32 devices in a mesh: dp: 4 (over y, core), vocab: 8 (over z, x).
Axes of the slice: x: 2, y: 2, z: 4, core: 2. Of those that a mesh axis runs over, the one named last changes fastest.
Arguments:
- hidden: bfloat16 [256, 3584], P('dp'), may hold values from -48 to 48
- embedding: bfloat16 [24576, 3584], P(('dp', 'vocab')), may hold values from -1 to 1
- targets: int32 [256], P('dp'), may hold values from 0 to 24575
- loss_weight: bfloat16 [256], P('dp'), may hold values from 1 to 10
Outputs:
- hidden_grad: bfloat16 [256, 3584], P('dp')
- table_grad: bfloat16 [24576, 3584], P(('dp', 'vocab'))
The draws below stay inside these ranges and needn't reach their ends.
All inputs are finite; a program needn't handle non-finite values.
Results may differ from the reference program's by a relative error of at most 0.0049.
Values may be sent and summed in bfloat16 or wider, within the bound.
No kernel may reach another device: no remote copies, remote signals or barrier semaphores. Data moves between devices by JAX's collectives and lax.ppermute only.
A program may use at most 128 MiB of HBM per device.

```python
import math
import jax
import jax.numpy as jnp
import numpy as np
from jax import lax

D = 3584
VROWS = 768
VOCAB = 24576
TOKENS = 256
N_VOCAB = 8


def draw_hidden(key, part):
    noise = jnp.clip(jax.random.normal(jax.random.fold_in(key, 11), (TOKENS, D), jnp.float32), -6.0, 6.0)
    return noise.astype(jnp.bfloat16)


def draw_embedding(key, part):
    noise = jnp.clip(jax.random.normal(jax.random.fold_in(key, 13), (VOCAB, D), jnp.float32), -6.0, 6.0)
    place = jnp.arange(VOCAB, dtype=jnp.float32) / (VOCAB - 1)
    rising = jnp.sqrt(1.0 + 0.245 * place)
    table = noise * (3.0 / math.sqrt(D))
    return jnp.clip(table * rising[:, None], -1.0, 1.0).astype(jnp.bfloat16)


def with_ends(drawn, stream_key, low, top_value):
    extent = drawn.shape
    spot = [jax.random.randint(jax.random.fold_in(stream_key, axis), (), 0, extent[axis]) for axis in range(len(extent))]
    drawn = drawn.at[tuple(spot)].set(low)
    longest = extent.index(max(extent))
    spot[longest] = (spot[longest] + 1) % extent[longest]
    return drawn.at[tuple(spot)].set(top_value)


def levels(own_key, dims, pieces, low, top_value):
    gain, own = 1.0, jax.random.fold_in(own_key, 6)
    for position, parts in pieces:
        draws = jnp.exp(jax.random.uniform(jax.random.fold_in(own, position), (parts,), jnp.float32, low / len(pieces), top_value / len(pieces)))
        gain = gain * jnp.repeat(draws, dims[position] // parts).reshape([-1 if axis == position else 1 for axis in range(len(dims))])
    return gain


def cumulative_ranks(amount, slope):
    weights = [(1 << 20) // math.isqrt(standing ** slope) + 1 for standing in range(1, amount + 1)]
    scale = 1 + sum(weights) // (1 << 30)
    return np.cumsum(np.array([max(1, weight // scale) for weight in weights]))


def ranked_ids(rng, extent, number_of, skew):
    table = cumulative_ranks(number_of, skew)
    pick = jax.random.randint(jax.random.fold_in(rng, 1), extent, 0, int(table[number_of - 1]))
    grade = jnp.searchsorted(jnp.asarray(table, jnp.int32), pick, side="right")
    return jax.random.permutation(jax.random.fold_in(rng, 2), number_of)[grade].astype(jnp.int32)


def setup_inputs(seed: int = 0) -> dict:
    keys = jax.random.split(jax.random.key(seed), 5)
    hidden = draw_hidden(jax.random.fold_in(keys[4], 71), 0)
    embedding = draw_embedding(jax.random.fold_in(keys[4], 71), 0)
    targets = with_ends(ranked_ids(keys[2], (TOKENS,), VOCAB, 2), jax.random.fold_in(keys[2], 3), 0, VOCAB - 1).astype(jnp.int32)
    loss_weight = jnp.clip(jnp.exp(math.log(10.0) - 2.3025851 * jax.random.uniform(keys[3], (TOKENS,), jnp.float32) ** levels(keys[3], (TOKENS,), ((0, 4),), -0.2, 0.2)), 1.0, 10.0).astype(jnp.bfloat16)
    return dict(hidden=hidden, embedding=embedding, targets=targets, loss_weight=loss_weight)


soft_cap = 30.0
z_weight = 0.002


def capped_block(hidden, table_rows):
    logits = lax.dot_general(hidden, table_rows, (((1,), (1,)), ((), ())), preferred_element_type=jnp.float32)
    return soft_cap * jnp.tanh(logits / soft_cap)


def reference(hidden, embedding, targets, loss_weight):
    block_rows = VROWS * N_VOCAB
    table_blocks = embedding.reshape(VOCAB // block_rows, block_rows, D)

    def add_exp(exp_total, table_rows):
        capped = capped_block(hidden, table_rows)
        return exp_total + jnp.sum(jnp.exp(capped - soft_cap), axis=1), None

    exp_total, _ = lax.scan(add_exp, jnp.zeros((hidden.shape[0],), jnp.float32), table_blocks)
    weight = loss_weight.astype(jnp.float32)
    log_total = soft_cap + jnp.log(exp_total)
    factor = weight * (1.0 + 2.0 * z_weight * log_total) / exp_total

    def grads(accum_grad, blocks_item):
        table_rows, first_row = blocks_item
        capped = capped_block(hidden, table_rows)
        columns = first_row + jnp.arange(block_rows, dtype=jnp.int32)
        target_hit = targets[:, None] == columns[None, :]
        softmax_part = factor[:, None] * jnp.exp(capped - soft_cap) - jnp.where(target_hit, weight[:, None], 0.0)
        scores_grad = (softmax_part * (1.0 - (capped / soft_cap) ** 2)).astype(jnp.bfloat16)
        accum_grad = accum_grad + jnp.dot(scores_grad, table_rows, preferred_element_type=jnp.float32)
        rows_grad = lax.dot_general(scores_grad, hidden, (((0,), (0,)), ((), ())), preferred_element_type=jnp.float32)
        return accum_grad, rows_grad.astype(jnp.bfloat16)

    first_rows = jnp.arange(VOCAB // block_rows, dtype=jnp.int32) * block_rows
    hidden_sum, block_grads = lax.scan(grads, jnp.zeros(hidden.shape, jnp.float32), (table_blocks, first_rows))
    return hidden_sum.astype(jnp.bfloat16), block_grads.reshape(VOCAB, D)
```

```python
import jax
import jax.numpy as jnp
from jax import lax
from jax.sharding import PartitionSpec as P

soft_cap = 30.0
z_weight = 0.002
bf16 = jnp.bfloat16
f32 = jnp.float32


def exchange(x, axis, bit):
    return lax.ppermute(x, axis, [(i, i ^ bit) for i in range(lax.axis_size(axis))])


def axis_bits(axis):
    size = lax.axis_size(axis)
    assert size & (size - 1) == 0
    return [1 << b for b in range(size.bit_length() - 1)]


def gather_relative(x):
    for bit in reversed(axis_bits("dp")):
        x = jnp.concatenate([x, exchange(x, "dp", bit)], axis=0)
    return x


def relative_to_absolute(x, inverse=False):
    size = lax.axis_size("dp")
    nbits = size.bit_length() - 1
    place = lax.axis_index("dp")
    x = x.reshape((2,) * nbits + (-1,))
    def flip(x):
        for b in range(nbits):
            hit = ((place >> b) & 1) == 1
            x = jnp.where(hit, lax.rev(x, (b,)), x)
        return x
    order = tuple(reversed(range(nbits))) + (nbits,)
    if inverse:
        return flip(x.transpose(order)).reshape(-1)
    return flip(x).transpose(order).reshape(-1)


def scatter_relative(x):
    for bit in axis_bits("dp"):
        half = x.shape[0] // 2
        other = exchange(x[half:].astype(bf16), "dp", bit)
        x = x[:half].astype(f32) + other.astype(f32)
    return x.astype(bf16)


def sum_over_vocab(x):
    size = lax.axis_size("vocab")
    rows = x.shape[0] // size
    parts = lax.all_to_all(x.reshape(size, rows, x.shape[1]), "vocab", 0, 0)
    total = jnp.sum(parts.astype(f32), axis=0).astype(bf16)
    spread = jnp.broadcast_to(total[None], (size,) + total.shape)
    return lax.all_to_all(spread, "vocab", 0, 0).reshape(x.shape)


def body(hidden, embedding, targets, loss_weight):
    shard_rows = embedding.shape[0]
    both = ("dp", "vocab")
    n_all = lax.axis_size("dp") * lax.axis_size("vocab")
    group_hidden = gather_relative(hidden)
    side = gather_relative(jnp.stack([loss_weight.astype(f32), targets.astype(f32)], axis=1))
    weight = side[:, :1]
    group_targets = side[:, 1:].astype(jnp.int32)
    logits = lax.dot_general(
        group_hidden, embedding, (((1,), (1,)), ((), ())), preferred_element_type=f32
    )
    capped = soft_cap * jnp.tanh(logits / soft_cap)
    exp_terms = jnp.exp(capped - soft_cap)
    partial_value = relative_to_absolute(jnp.sum(exp_terms, axis=1))
    spread = jnp.broadcast_to(partial_value[None], (n_all,) + partial_value.shape)
    exp_total = jnp.sum(lax.all_to_all(spread, both, 0, 0), axis=0)
    exp_total = relative_to_absolute(exp_total, inverse=True)[:, None]
    factor = weight * (1.0 + 2.0 * z_weight * (soft_cap + jnp.log(exp_total))) / exp_total
    columns = lax.axis_index(both) * shard_rows + lax.iota(jnp.int32, shard_rows)
    target_hit = group_targets == columns[None, :]
    softmax_part = factor * exp_terms - jnp.where(target_hit, weight, 0.0)
    scores_grad = (softmax_part * (1.0 - (capped / soft_cap) ** 2)).astype(bf16)
    group_grad = jnp.dot(scores_grad, embedding, preferred_element_type=f32)
    hidden_grad = sum_over_vocab(scatter_relative(group_grad))
    table_grad = lax.dot_general(
        scores_grad, group_hidden, (((0,), (0,)), ((), ())), preferred_element_type=f32
    ).astype(bf16)
    return (hidden_grad, table_grad)


def solution(mesh):
    return jax.shard_map(
        body,
        mesh=mesh,
        in_specs=(P("dp", None), P(("dp", "vocab"), None), P("dp"), P("dp")),
        out_specs=(P("dp", None), P(("dp", "vocab"), None)),
        check_vma=False,
    )
```

```python
import jax
import jax.numpy as jnp
from jax import lax
from jax.sharding import PartitionSpec as P

soft_cap = 30.0
z_weight = 0.002
bf16 = jnp.bfloat16
f32 = jnp.float32


def exchange(x, axis, bit):
    return lax.ppermute(x, axis, [(i, i ^ bit) for i in range(lax.axis_size(axis))])


def axis_bits(axis):
    size = lax.axis_size(axis)
    assert size & (size - 1) == 0
    return [1 << b for b in range(size.bit_length() - 1)]


def gather_relative(x):
    near, *far = axis_bits("dp")
    pieces = [x]
    for bit in reversed(far):
        pieces = pieces + [exchange(p, "dp", bit) for p in pieces]
    return jnp.concatenate(pieces + [exchange(p, "dp", near) for p in pieces], axis=0)


def relative_to_absolute(x, inverse=False):
    size = lax.axis_size("dp")
    nbits = size.bit_length() - 1
    place = lax.axis_index("dp")
    x = x.reshape((2,) * nbits + (-1,))
    def flip(x):
        for b in range(nbits):
            hit = ((place >> b) & 1) == 1
            x = jnp.where(hit, lax.rev(x, (b,)), x)
        return x
    order = tuple(reversed(range(nbits))) + (nbits,)
    if inverse:
        return flip(x.transpose(order)).reshape(-1)
    return flip(x).transpose(order).reshape(-1)


def take(x, index, rows, axis=0):
    return lax.dynamic_slice_in_dim(x, index * rows, rows, axis)


def halve(x, bit):
    half = x.shape[0] // 2
    other = exchange(x[half:].astype(bf16), "dp", bit)
    return x[:half].astype(f32) + other.astype(f32)


def halve_vocab(x, blocks):
    place = lax.axis_index("vocab") % 2
    half = x.shape[0] // (2 * blocks)
    x = x.reshape(blocks, 2 * half, x.shape[1])
    other = exchange(take(x, 1 - place, half, 1).astype(bf16), "vocab", 1)
    return (take(x, place, half, 1).astype(f32) + other.astype(f32)).reshape(blocks * half, -1)


def shift_pairs(x, k):
    size = lax.axis_size("vocab")
    return lax.ppermute(x, "vocab", [(i, (i + 2 * k) % size) for i in range(size)])


def hops(count):
    return sorted(range(1, count), key=lambda k: -min(k, count - k))


def reduce_hidden(left, right):
    near, *far = axis_bits("dp")
    left, right = halve(left, near), halve(right, near)
    blocks = lax.axis_size("dp") // 2
    right = halve_vocab(right, blocks)
    for bit in far:
        left = halve(left, bit)
        right = halve(right, bit)
    left = halve_vocab(left, 1)
    part = jnp.concatenate([left, right], axis=1)
    count = lax.axis_size("vocab") // 2
    place = lax.axis_index("vocab") // 2
    rows = part.shape[0] // count
    total = take(part, place, rows)
    sent = part.astype(bf16)
    for k in hops(count):
        total = total + shift_pairs(take(sent, (place + k) % count, rows), k).astype(f32)
    total = total.astype(bf16)
    out = jnp.zeros(part.shape, bf16)
    for k, piece in [(0, total)] + [(k, shift_pairs(total, k)) for k in hops(count)]:
        out = lax.dynamic_update_slice_in_dim(out, piece, ((place - k) % count) * rows, 0)
    other = exchange(out, "vocab", 1)
    low = lax.axis_index("vocab") % 2 == 0
    return jnp.where(low, jnp.concatenate([out, other], 0), jnp.concatenate([other, out], 0))


def body(hidden, embedding, targets, loss_weight):
    shard_rows = embedding.shape[0]
    both = ("dp", "vocab")
    n_all = lax.axis_size("dp") * lax.axis_size("vocab")
    group_hidden = gather_relative(hidden)
    side = gather_relative(jnp.stack([loss_weight.astype(f32), targets.astype(f32)], axis=1))
    weight = side[:, :1]
    group_targets = side[:, 1:].astype(jnp.int32)
    logits = lax.dot_general(
        group_hidden, embedding, (((1,), (1,)), ((), ())), preferred_element_type=f32
    )
    capped = soft_cap * jnp.tanh(logits / soft_cap)
    exp_terms = jnp.exp(capped - soft_cap)
    partial_value = relative_to_absolute(jnp.sum(exp_terms, axis=1))
    spread = jnp.broadcast_to(partial_value[None], (n_all,) + partial_value.shape)
    totals = lax.all_to_all(spread, both, 0, 0)
    columns = lax.axis_index(both) * shard_rows + lax.iota(jnp.int32, shard_rows)
    hit_weight = jnp.where(group_targets == columns[None, :], weight, 0.0)
    slope = 1.0 - (capped / soft_cap) ** 2
    exp_total = relative_to_absolute(jnp.sum(totals, axis=0), inverse=True)[:, None]
    factor = weight * (1.0 + 2.0 * z_weight * (soft_cap + jnp.log(exp_total))) / exp_total
    scores_grad = ((factor * exp_terms - hit_weight) * slope).astype(bf16)
    cut = embedding.shape[1] // 2
    left = jnp.dot(scores_grad, embedding[:, :cut], preferred_element_type=f32)
    right = jnp.dot(scores_grad, embedding[:, cut:], preferred_element_type=f32)
    hidden_grad = reduce_hidden(left, right)
    table_grad = lax.dot_general(
        scores_grad, group_hidden, (((0,), (0,)), ((), ())), preferred_element_type=f32
    ).astype(bf16)
    return (hidden_grad, table_grad)


def solution(mesh):
    return jax.shard_map(
        body,
        mesh=mesh,
        in_specs=(P("dp", None), P(("dp", "vocab"), None), P("dp"), P("dp")),
        out_specs=(P("dp", None), P(("dp", "vocab"), None)),
        check_vma=False,
    )
```

```python
import jax
import jax.numpy as jnp
from jax import lax
from jax.sharding import PartitionSpec as P

soft_cap = 30.0
z_weight = 0.002
bf16 = jnp.bfloat16
f32 = jnp.float32


def exchange(x, axis, bit):
    return lax.ppermute(x, axis, [(i, i ^ bit) for i in range(lax.axis_size(axis))])


def axis_bits(axis):
    size = lax.axis_size(axis)
    assert size & (size - 1) == 0
    return [1 << b for b in range(size.bit_length() - 1)]


def gather_relative(x):
    near, *far = axis_bits("dp")
    pieces = [x]
    for bit in reversed(far):
        pieces = pieces + [exchange(p, "dp", bit) for p in pieces]
    return jnp.concatenate(pieces + [exchange(p, "dp", near) for p in pieces], axis=0)


def relative_to_absolute(x, inverse=False):
    size = lax.axis_size("dp")
    nbits = size.bit_length() - 1
    place = lax.axis_index("dp")
    x = x.reshape((2,) * nbits + (-1,))
    def flip(x):
        for b in range(nbits):
            hit = ((place >> b) & 1) == 1
            x = jnp.where(hit, lax.rev(x, (b,)), x)
        return x
    order = tuple(reversed(range(nbits))) + (nbits,)
    if inverse:
        return flip(x.transpose(order)).reshape(-1)
    return flip(x).transpose(order).reshape(-1)


def take(x, index, rows, axis=0):
    return lax.dynamic_slice_in_dim(x, index * rows, rows, axis)


def halve(x, bit):
    half = x.shape[0] // 2
    other = exchange(x[half:].astype(bf16), "dp", bit)
    return x[:half].astype(f32) + other.astype(f32)


def halve_vocab(x, blocks):
    place = lax.axis_index("vocab") % 2
    half = x.shape[0] // (2 * blocks)
    x = x.reshape(blocks, 2 * half, x.shape[1])
    other = exchange(take(x, 1 - place, half, 1).astype(bf16), "vocab", 1)
    return (take(x, place, half, 1).astype(f32) + other.astype(f32)).reshape(blocks * half, -1)


def reduce_hidden(left, right):
    near, *far = axis_bits("dp")
    left, right = halve(left, near), halve(right, near)
    blocks = lax.axis_size("dp") // 2
    right = halve_vocab(right, blocks)
    for bit in far:
        left = halve(left, bit)
        right = halve(right, bit)
    left = halve_vocab(left, 1)
    part = jnp.concatenate([left, right], axis=1)
    for bit in axis_bits("vocab")[1:]:
        part = part + exchange(part.astype(bf16), "vocab", bit).astype(f32)
    out = part.astype(bf16)
    other = exchange(out, "vocab", 1)
    low = lax.axis_index("vocab") % 2 == 0
    return jnp.where(low, jnp.concatenate([out, other], 0), jnp.concatenate([other, out], 0))


def body(hidden, embedding, targets, loss_weight):
    shard_rows = embedding.shape[0]
    both = ("dp", "vocab")
    n_all = lax.axis_size("dp") * lax.axis_size("vocab")
    group_hidden = gather_relative(hidden)
    side = gather_relative(jnp.stack([loss_weight.astype(f32), targets.astype(f32)], axis=1))
    weight = side[:, :1]
    group_targets = side[:, 1:].astype(jnp.int32)
    logits = lax.dot_general(
        group_hidden, embedding, (((1,), (1,)), ((), ())), preferred_element_type=f32
    )
    capped = soft_cap * jnp.tanh(logits / soft_cap)
    exp_terms = jnp.exp(capped - soft_cap)
    partial_value = relative_to_absolute(jnp.sum(exp_terms, axis=1))
    spread = jnp.broadcast_to(partial_value[None], (n_all,) + partial_value.shape)
    totals = lax.all_to_all(spread, both, 0, 0)
    columns = lax.axis_index(both) * shard_rows + lax.iota(jnp.int32, shard_rows)
    hit_weight = jnp.where(group_targets == columns[None, :], weight, 0.0)
    slope = 1.0 - (capped / soft_cap) ** 2
    exp_total = relative_to_absolute(jnp.sum(totals, axis=0), inverse=True)[:, None]
    factor = weight * (1.0 + 2.0 * z_weight * (soft_cap + jnp.log(exp_total))) / exp_total
    scores_grad = ((factor * exp_terms - hit_weight) * slope).astype(bf16)
    cut = embedding.shape[1] // 2
    left = jnp.dot(scores_grad, embedding[:, :cut], preferred_element_type=f32)
    right = jnp.dot(scores_grad, embedding[:, cut:], preferred_element_type=f32)
    hidden_grad = reduce_hidden(left, right)
    table_grad = lax.dot_general(
        scores_grad, group_hidden, (((0,), (0,)), ((), ())), preferred_element_type=f32
    ).astype(bf16)
    return (hidden_grad, table_grad)


def solution(mesh):
    return jax.shard_map(
        body,
        mesh=mesh,
        in_specs=(P("dp", None), P(("dp", "vocab"), None), P("dp"), P("dp")),
        out_specs=(P("dp", None), P(("dp", "vocab"), None)),
        check_vma=False,
    )
```
